32 devices in a mesh: hp: 4 (over x, y), cp: 8 (over z, core).
Axes of the slice: x: 2, y: 2, z: 4, core: 2. Of those that a mesh axis runs over, the one named last changes fastest.
Arguments:
- q_heads: bfloat16 [8192, 48, 128], P('cp', 'hp'), parts along dimension 1
- k_heads: bfloat16 [8192, 48, 128], P('cp', 'hp'), parts along dimension 1
- v_heads: bfloat16 [8192, 48, 128], P('cp', 'hp'), parts along dimension 1
- o_heads: bfloat16 [8192, 48, 128], P('cp', 'hp'), parts along dimension 1
- do_heads: bfloat16 [8192, 48, 128], P('cp', 'hp'), parts along dimension 1
- lse_rows: float32 [8192, 48], P('cp', 'hp'), parts along dimension 1
- cu_seqlens: int32 [67], replicated
Outputs:
- output 1: bfloat16 [8192, 48, 128], P('cp', 'hp'), parts along dimension 1
- output 2: bfloat16 [8192, 48, 128], P('cp', 'hp'), parts along dimension 1
- output 3: bfloat16 [8192, 48, 128], P('cp', 'hp'), parts along dimension 1
There are 4 independent parts. The reference program is written for one: setup_inputs(seed, part) draws one part's arguments, and reference() takes and returns one part's arrays. A program takes and returns all parts, laid end to end along the dimension named above; an argument that names none is the same for every part.
All inputs are finite; a program needn't handle non-finite values.
Results may differ from the reference program's by a relative error of at most 0.001.
Values are sent between devices in bfloat16 or wider.
A program may use at most 1 GiB of HBM per device.

```python
import jax
import jax.numpy as jnp
from jax import lax

CHUNK_LEN = 1024
CP_SIZE = 8
HEADS_LOCAL = 12
HEAD_DIM = 128
REACH_CHUNKS = 3
QBLOCK = 256

SEQ_LEN = CHUNK_LEN * CP_SIZE
DOC_SLOTS = 8 * CP_SIZE + 2
WINDOW = REACH_CHUNKS * CHUNK_LEN
SOFTMAX_SCALE = HEAD_DIM ** -0.5
N_BLOCKS = SEQ_LEN // QBLOCK


def draw_cu_seqlens(doc_key):
    key_first, key_base, key_tier, key_long = jax.random.split(doc_key, 4)
    first_len = CHUNK_LEN // 4 + jax.random.randint(key_first, (1,), 0, CHUNK_LEN // 2)
    base_len = jax.random.randint(key_base, (DOC_SLOTS - 2,), CHUNK_LEN // 8, CHUNK_LEN + 1)
    long_len = WINDOW - jax.random.randint(key_long, (DOC_SLOTS - 2,), 0, CHUNK_LEN)
    tier_draw = jax.random.randint(key_tier, (DOC_SLOTS - 2,), 0, 4)
    rest_len = jnp.where(tier_draw == 3, long_len, base_len * jnp.where(tier_draw == 2, 2, 1))
    lengths = jnp.concatenate([first_len, jnp.full((1,), WINDOW, jnp.int32), rest_len]).astype(jnp.int32)
    doc_ends = jnp.minimum(jnp.cumsum(lengths), SEQ_LEN).astype(jnp.int32)
    return jnp.concatenate([jnp.zeros((1,), jnp.int32), doc_ends])


def doc_index(cu_seqlens):
    positions = jnp.arange(SEQ_LEN, dtype=jnp.int32)
    return (jnp.searchsorted(cu_seqlens, positions, side="right") - 1).astype(jnp.int32)


def window_mask(q_doc, q_pos, k_doc, k_pos):
    return (q_doc[:, None] == k_doc[None, :]) & (k_pos[None, :] <= q_pos[:, None])


def attention_forward(q_heads, k_heads, v_heads, doc_ids):
    front_pad = jnp.zeros((WINDOW, HEADS_LOCAL, HEAD_DIM), jnp.float32)
    k_pad = jnp.concatenate([front_pad, k_heads.astype(jnp.float32)])
    v_pad = jnp.concatenate([front_pad, v_heads.astype(jnp.float32)])
    doc_pad = jnp.concatenate([jnp.full((WINDOW,), -1, jnp.int32), doc_ids])
    q_full = q_heads.astype(jnp.float32)

    def forward_block(blk_idx):
        q_start = blk_idx * QBLOCK
        q_pos = q_start + jnp.arange(QBLOCK, dtype=jnp.int32)
        k_pos = q_start - WINDOW + jnp.arange(WINDOW + QBLOCK, dtype=jnp.int32)
        keep_mask = window_mask(lax.dynamic_slice_in_dim(doc_ids, q_start, QBLOCK), q_pos, lax.dynamic_slice_in_dim(doc_pad, q_start, WINDOW + QBLOCK), k_pos)
        q_blk = lax.dynamic_slice_in_dim(q_full, q_start, QBLOCK)
        k_win = lax.dynamic_slice_in_dim(k_pad, q_start, WINDOW + QBLOCK)
        v_win = lax.dynamic_slice_in_dim(v_pad, q_start, WINDOW + QBLOCK)
        scores = jnp.einsum("qhd,khd->hqk", q_blk, k_win) * SOFTMAX_SCALE
        scores = jnp.where(keep_mask[None], scores, -jnp.inf)
        row_max = jnp.max(scores, axis=-1, keepdims=True)
        weights = jnp.exp(scores - row_max)
        row_sum = jnp.sum(weights, axis=-1, keepdims=True)
        out_blk = jnp.einsum("hqk,khd->qhd", weights / row_sum, v_win)
        lse_blk = jnp.transpose((row_max + jnp.log(row_sum))[:, :, 0])
        return out_blk.astype(jnp.bfloat16), lse_blk

    out_blocks, lse_blocks = lax.map(forward_block, jnp.arange(N_BLOCKS))
    return out_blocks.reshape(SEQ_LEN, HEADS_LOCAL, HEAD_DIM), lse_blocks.reshape(SEQ_LEN, HEADS_LOCAL)


def setup_inputs(seed: int = 0, part: int = 0) -> dict:
    doc_key, data_key = jax.random.split(jax.random.key(seed))
    cu_seqlens = draw_cu_seqlens(doc_key)
    doc_ids = doc_index(cu_seqlens)
    key_q, key_k, key_v, key_do = jax.random.split(jax.random.fold_in(data_key, part), 4)
    head_shape = (SEQ_LEN, HEADS_LOCAL, HEAD_DIM)
    q_heads = jax.random.normal(key_q, head_shape, jnp.float32).astype(jnp.bfloat16)
    k_heads = jax.random.normal(key_k, head_shape, jnp.float32).astype(jnp.bfloat16)
    v_heads = jax.random.normal(key_v, head_shape, jnp.float32).astype(jnp.bfloat16)
    do_heads = (jax.random.normal(key_do, head_shape, jnp.float32) * (0.5 * CHUNK_LEN ** 0.5)).astype(jnp.bfloat16)
    o_heads, lse_rows = attention_forward(q_heads, k_heads, v_heads, doc_ids)
    return {"q_heads": q_heads, "k_heads": k_heads, "v_heads": v_heads, "o_heads": o_heads, "do_heads": do_heads, "lse_rows": lse_rows, "cu_seqlens": cu_seqlens}


def reference(q_heads, k_heads, v_heads, o_heads, do_heads, lse_rows, cu_seqlens):
    doc_ids = doc_index(cu_seqlens)
    q_full = q_heads.astype(jnp.float32)
    k_full = k_heads.astype(jnp.float32)
    v_full = v_heads.astype(jnp.float32)
    do_full = do_heads.astype(jnp.float32)
    delta_rows = jnp.sum(do_full * o_heads.astype(jnp.float32), axis=-1)
    zero_rows = jnp.zeros((WINDOW, HEADS_LOCAL, HEAD_DIM), jnp.float32)
    zero_stats = jnp.zeros((WINDOW, HEADS_LOCAL), jnp.float32)
    no_doc = jnp.full((WINDOW,), -1, jnp.int32)
    k_front = jnp.concatenate([zero_rows, k_full])
    v_front = jnp.concatenate([zero_rows, v_full])
    doc_front = jnp.concatenate([no_doc, doc_ids])
    q_back = jnp.concatenate([q_full, zero_rows])
    do_back = jnp.concatenate([do_full, zero_rows])
    lse_back = jnp.concatenate([lse_rows, zero_stats])
    delta_back = jnp.concatenate([delta_rows, zero_stats])
    doc_back = jnp.concatenate([doc_ids, no_doc])

    def dq_block(blk_idx):
        q_start = blk_idx * QBLOCK
        q_pos = q_start + jnp.arange(QBLOCK, dtype=jnp.int32)
        k_pos = q_start - WINDOW + jnp.arange(WINDOW + QBLOCK, dtype=jnp.int32)
        keep_mask = window_mask(lax.dynamic_slice_in_dim(doc_ids, q_start, QBLOCK), q_pos, lax.dynamic_slice_in_dim(doc_front, q_start, WINDOW + QBLOCK), k_pos)
        q_blk = lax.dynamic_slice_in_dim(q_full, q_start, QBLOCK)
        do_blk = lax.dynamic_slice_in_dim(do_full, q_start, QBLOCK)
        lse_blk = lax.dynamic_slice_in_dim(lse_rows, q_start, QBLOCK)
        delta_blk = lax.dynamic_slice_in_dim(delta_rows, q_start, QBLOCK)
        k_win = lax.dynamic_slice_in_dim(k_front, q_start, WINDOW + QBLOCK)
        v_win = lax.dynamic_slice_in_dim(v_front, q_start, WINDOW + QBLOCK)
        scores = jnp.einsum("qhd,khd->hqk", q_blk, k_win)
        p_matrix = jnp.exp(jnp.where(keep_mask[None], scores * SOFTMAX_SCALE - lse_blk.T[:, :, None], -jnp.inf))
        dprobs = jnp.einsum("qhd,khd->hqk", do_blk, v_win)
        dscores = (p_matrix * (dprobs - delta_blk.T[:, :, None])).astype(jnp.bfloat16).astype(jnp.float32)
        return jnp.einsum("hqk,khd->qhd", dscores, k_win) * SOFTMAX_SCALE

    def dkv_block(blk_idx):
        k_start = blk_idx * QBLOCK
        k_pos = k_start + jnp.arange(QBLOCK, dtype=jnp.int32)
        q_pos = k_start + jnp.arange(QBLOCK + WINDOW, dtype=jnp.int32)
        keep_mask = window_mask(lax.dynamic_slice_in_dim(doc_back, k_start, QBLOCK + WINDOW), q_pos, lax.dynamic_slice_in_dim(doc_ids, k_start, QBLOCK), k_pos)
        q_win = lax.dynamic_slice_in_dim(q_back, k_start, QBLOCK + WINDOW)
        do_win = lax.dynamic_slice_in_dim(do_back, k_start, QBLOCK + WINDOW)
        lse_win = lax.dynamic_slice_in_dim(lse_back, k_start, QBLOCK + WINDOW)
        delta_win = lax.dynamic_slice_in_dim(delta_back, k_start, QBLOCK + WINDOW)
        k_blk = lax.dynamic_slice_in_dim(k_full, k_start, QBLOCK)
        v_blk = lax.dynamic_slice_in_dim(v_full, k_start, QBLOCK)
        scores = jnp.einsum("qhd,khd->hqk", q_win, k_blk)
        p_matrix = jnp.exp(jnp.where(keep_mask[None], scores * SOFTMAX_SCALE - lse_win.T[:, :, None], -jnp.inf))
        dv_blk = jnp.einsum("hqk,qhd->khd", p_matrix.astype(jnp.bfloat16).astype(jnp.float32), do_win)
        dprobs = jnp.einsum("qhd,khd->hqk", do_win, v_blk)
        dscores = (p_matrix * (dprobs - delta_win.T[:, :, None])).astype(jnp.bfloat16).astype(jnp.float32)
        dk_blk = jnp.einsum("hqk,qhd->khd", dscores, q_win) * SOFTMAX_SCALE
        return dk_blk, dv_blk

    full_shape = (SEQ_LEN, HEADS_LOCAL, HEAD_DIM)
    dq_blocks = lax.map(dq_block, jnp.arange(N_BLOCKS))
    dk_blocks, dv_blocks = lax.map(dkv_block, jnp.arange(N_BLOCKS))
    return (dq_blocks.reshape(full_shape).astype(jnp.bfloat16), dk_blocks.reshape(full_shape).astype(jnp.bfloat16), dv_blocks.reshape(full_shape).astype(jnp.bfloat16))
```

```python
import functools
import math

import jax
import jax.numpy as jnp
from jax import lax
from jax.experimental import pallas as pl
from jax.experimental.pallas import tpu as pltpu
from jax.sharding import PartitionSpec as P

LOG2E = math.log2(math.e)
MAX_DOC = 3072
QB = 256
KB = 256
GROUPS = (2, 2, 2)
NT = (((1,), (1,)), ((), ()))
NN = (((1,), (0,)), ((), ()))
TN = (((0,), (0,)), ((), ()))


def mm(a, b, dims):
    return lax.dot_general(a, b, dims, preferred_element_type=jnp.float32)


def attn_kernel(tok, reach, scale, tab, q, k, v, do, st, qs, kvu, qdd, std, qsd, *rest):
    dq, dk, dv, dq_acc, dk_acc, dv_acc = rest[-6:]
    nq, nk, nu, nd = tok // QB, tok // KB, reach // KB, reach // QB
    half = tok // 2
    qh, kh = half // QB, half // KB
    base = tab[0]
    c1 = scale * LOG2E
    dq_acc[...] = jnp.zeros_like(dq_acc)
    dk_acc[...] = jnp.zeros_like(dk_acc)
    dv_acc[...] = jnp.zeros_like(dv_acc)

    def terms(kb, vb, qb, dob, rows, starts, k_pos, q_pos):
        s = mm(kb, qb, NT)
        kp = k_pos + lax.broadcasted_iota(jnp.int32, (KB, QB), 0)
        vis = kp >= starts
        if q_pos is not None:
            vis = vis & (kp <= q_pos + lax.broadcasted_iota(jnp.int32, (KB, QB), 1))
        p = jnp.where(vis, jnp.exp2(s * c1 - rows[0:1, :]), 0.0)
        dp = mm(vb, dob, NT)
        ds = (p * (dp - rows[1:2, :])).astype(jnp.bfloat16)
        return p.astype(jnp.bfloat16), ds

    def local_q(i, _):
        hi_q, lo_q = i // qh, lax.rem(i, qh)
        qsl = pl.ds(pl.multiple_of(lo_q * QB, QB), QB)
        asl = pl.ds(pl.multiple_of(i * QB, QB), QB)

        def up_k(j, _):
            sl = pl.ds(pl.multiple_of(j * KB, KB), KB)
            kb = kvu[0, 0, sl, :]
            _, ds = terms(kb, kvu[1, 0, sl, :], q[hi_q, 0, qsl, :], do[hi_q, 0, qsl, :], st[0, i], qs[i], base - reach + j * KB, None)
            dq_acc[asl, :] += mm(ds, kb, TN)
            return 0

        def local_k(j, _):
            hi_k, lo_k = j // kh, lax.rem(j, kh)
            sl = pl.ds(pl.multiple_of(lo_k * KB, KB), KB)
            ksl = pl.ds(pl.multiple_of(j * KB, KB), KB)
            kb = k[hi_k, 0, sl, :]
            qb, dob = q[hi_q, 0, qsl, :], do[hi_q, 0, qsl, :]
            p, ds = terms(kb, v[hi_k, 0, sl, :], qb, dob, st[0, i], qs[i], base + j * KB, base + i * QB)
            dv_acc[ksl, :] += mm(p, dob, NN)
            dk_acc[ksl, :] += mm(ds, qb, NN)
            dq_acc[asl, :] += mm(ds, kb, TN)
            return 0

        lax.fori_loop(tab[1 + i], nu, up_k, 0)
        lax.fori_loop(tab[1 + nq + i], (i * QB + QB - 1) // KB + 1, local_k, 0)
        return 0

    lax.fori_loop(0, nq, local_q, 0)

    def down_q(i, _):
        qsl = pl.ds(pl.multiple_of(i * QB, QB), QB)

        def down_k(j, _):
            hi_k, lo_k = j // kh, lax.rem(j, kh)
            sl = pl.ds(pl.multiple_of(lo_k * KB, KB), KB)
            ksl = pl.ds(pl.multiple_of(j * KB, KB), KB)
            qb, dob = qdd[0, 0, qsl, :], qdd[1, 0, qsl, :]
            p, ds = terms(k[hi_k, 0, sl, :], v[hi_k, 0, sl, :], qb, dob, std[0, i], qsd[i], base + j * KB, None)
            dv_acc[ksl, :] += mm(p, dob, NN)
            dk_acc[ksl, :] += mm(ds, qb, NN)
            return 0

        lax.fori_loop(tab[1 + 2 * nq + i], nk, down_k, 0)
        return 0

    lax.fori_loop(0, nd, down_q, 0)
    for part in range(2):
        rows = slice(part * half, (part + 1) * half)
        dq[part, 0] = (dq_acc[rows, :] * scale).astype(jnp.bfloat16)
        dk[part, 0] = (dk_acc[rows, :] * scale).astype(jnp.bfloat16)
        dv[part, 0] = dv_acc[rows, :].astype(jnp.bfloat16)


def attn_call(tab, local, stats, starts, kvu, qdd, stats_d, starts_d, prev, h0):
    _, heads, half, dim = local[0].shape
    g, reach = kvu.shape[1], kvu.shape[2]
    tok = 2 * half
    nq, nd = tok // QB, reach // QB
    loc = pl.BlockSpec((2, 1, half, dim), lambda h, t: (0, h + h0, 0, 0))
    rem = pl.BlockSpec((2, 1, reach, dim), lambda h, t: (0, h, 0, 0))
    any_spec = pl.BlockSpec(memory_space=pl.ANY)
    in_specs = [loc] * 4 + [
        pl.BlockSpec((1, nq, 2, QB), lambda h, t: (h + h0, 0, 0, 0)),
        pl.BlockSpec((nq, 1, QB), lambda h, t: (0, 0, 0)),
        rem, rem,
        pl.BlockSpec((1, nd, 2, QB), lambda h, t: (h + h0, 0, 0, 0)),
        pl.BlockSpec((nd, 1, QB), lambda h, t: (0, 0, 0)),
    ] + [any_spec] * len(prev)
    n_in = 1 + 10
    flops = int(g * tok * tok * dim * 10)
    return pl.pallas_call(
        functools.partial(attn_kernel, tok, reach, dim ** -0.5),
        grid_spec=pltpu.PrefetchScalarGridSpec(
            num_scalar_prefetch=1, grid=(g,), in_specs=in_specs, out_specs=[loc] * 3,
            scratch_shapes=[pltpu.VMEM((tok, dim), jnp.float32)] * 3),
        out_shape=[jax.ShapeDtypeStruct((2, heads, half, dim), jnp.bfloat16)] * 3,
        input_output_aliases={n_in + i: i for i in range(len(prev))},
        compiler_params=pltpu.CompilerParams(dimension_semantics=("arbitrary",), vmem_limit_bytes=40 * 2**20),
        cost_estimate=pl.CostEstimate(flops=flops, bytes_accessed=g * 14 * tok * dim, transcendentals=0),
        name="attn",
    )(tab, *local, stats, starts, kvu, qdd, stats_d, starts_d, *prev)


def solution(mesh):
    cp = mesh.shape["cp"]
    chips = cp // 2
    head_spec = P("cp", "hp", None)
    pairs = [[2 * z, 2 * z + 1] for z in range(chips)]

    def device_fn(q_loc, k_loc, v_loc, o_loc, do_loc, lse_loc, cu):
        half, heads, dim = q_loc.shape
        hh = heads // 2
        tok = 2 * half
        seq = half * cp
        me = lax.axis_index("cp")
        base = (me // 2) * tok

        def gather(x):
            return lax.all_to_all(x.reshape((2, hh) + x.shape[1:]), "cp", 0, 0, axis_index_groups=pairs)

        def perm(x, hop, up):
            s = hop if up else -hop
            return lax.ppermute(x, "cp", [(2 * z + c, 2 * (z + s) + c) for z in range(chips) if 0 <= z + s < chips for c in range(2)])

        qh, kh, vh, oh, doh = (jnp.transpose(x, (1, 0, 2)) for x in (q_loc, k_loc, v_loc, o_loc, do_loc))
        lse = jnp.transpose(lse_loc)
        delta = jnp.sum(doh.astype(jnp.float32) * oh.astype(jnp.float32), axis=-1)

        pos = base + jnp.arange(tok + MAX_DOC, dtype=jnp.int32)
        start = jnp.max(jnp.where(cu[None, :] <= pos[:, None], cu[None, :], 0), axis=1)
        start = jnp.where(pos < seq, start, seq).astype(jnp.int32)

        def tables(reach):
            first = start[: tok + reach].reshape(-1, QB)[:, 0]
            loc_first, dn_first = first[: tok // QB], first[tok // QB :]
            lo_up = jnp.clip((loc_first - base + reach) // KB, 0, reach // KB)
            lo_loc = jnp.clip((loc_first - base) // KB, 0, tok // KB)
            lo_dn = jnp.clip((dn_first - base) // KB, 0, tok // KB)
            return jnp.concatenate([base[None], lo_up, lo_loc, lo_dn]).astype(jnp.int32)

        k2, v2, q2, do2 = gather(kh), gather(vh), gather(qh), gather(doh)
        st2 = gather(jnp.stack([lse * LOG2E, delta], axis=1))
        st_all = jnp.transpose(st2, (1, 2, 0, 3)).reshape(hh, 2, tok)

        def path(n, far):
            reach = n + far

            def last(x, h0, g, m):
                full = jnp.concatenate([x[0, h0 : h0 + g], x[1, h0 : h0 + g]], axis=1)
                return full[:, tok - m :]

            def head(x, h0, g, m):
                full = jnp.concatenate([x[0, h0 : h0 + g], x[1, h0 : h0 + g]], axis=1)
                return full[:, :m]

            st_dn = perm(st_all[:, :, :n], 1, False)
            if far:
                st_dn = jnp.concatenate([st_dn, perm(st_all[:, :, :far], 2, False)], axis=2)
            blocks = lambda x: jnp.transpose(x.reshape(hh, 2, -1, QB), (0, 2, 1, 3))
            stats, stats_d = blocks(st_all), blocks(st_dn)
            starts = start[:tok].reshape(-1, 1, QB)
            starts_d = start[tok : tok + reach].reshape(-1, 1, QB)
            tab = tables(reach)
            h0 = 0
            recv = []
            for g in GROUPS:
                kvu = perm(jnp.stack([last(k2, h0, g, n), last(v2, h0, g, n)]), 1, True)
                qdd = perm(jnp.stack([head(q2, h0, g, n), head(do2, h0, g, n)]), 1, False)
                if far:
                    kvf = perm(jnp.stack([last(k2, h0, g, far), last(v2, h0, g, far)]), 2, True)
                    qdf = perm(jnp.stack([head(q2, h0, g, far), head(do2, h0, g, far)]), 2, False)
                    kvu = jnp.concatenate([kvf, kvu], axis=2)
                    qdd = jnp.concatenate([qdd, qdf], axis=2)
                recv.append((kvu, qdd))
                h0 += g
            prev = ()
            h0 = 0
            for g, (kvu, qdd) in zip(GROUPS, recv):
                prev = attn_call(tab, (q2, k2, v2, do2), stats, starts, kvu, qdd, stats_d, starts_d, prev, h0)
                h0 += g
            return tuple(prev)

        edge = tok * jnp.arange(1, chips, dtype=jnp.int32)
        e_start = jnp.max(jnp.where(cu[None, :] < edge[:, None], cu[None, :], 0), axis=1)
        e_end = jnp.min(jnp.where(cu[None, :] >= edge[:, None], cu[None, :], seq), axis=1)
        e_start = jnp.where(e_end > edge, e_start, edge)
        need = jnp.max(jnp.maximum(edge - e_start, e_end - edge))
        branch = (need > 1792).astype(jnp.int32) + (need > tok).astype(jnp.int32)
        outs = lax.switch(branch, [lambda: path(1792, 0), lambda: path(tok, 0), lambda: path(tok, MAX_DOC - tok)])

        def back(x):
            y = lax.all_to_all(x, "cp", 0, 0, axis_index_groups=pairs)
            return jnp.transpose(y.reshape(heads, half, dim), (1, 0, 2))

        return tuple(back(x) for x in outs)

    specs = (head_spec,) * 5 + (P("cp", "hp"), P())
    return jax.shard_map(device_fn, mesh=mesh, in_specs=specs, out_specs=(head_spec,) * 3, check_vma=False)
```

```python
import functools
import math

import jax
import jax.numpy as jnp
from jax import lax
from jax.experimental import pallas as pl
from jax.experimental.pallas import tpu as pltpu
from jax.sharding import PartitionSpec as P

LOG2E = math.log2(math.e)
MAX_DOC = 3072
QB = 512
KB = 512
QBD = 256
UNROLL = (2, 2, 4)
GROUPS = (2, 2, 1, 1)
NARROW = 1792
NT = (((1,), (1,)), ((), ()))
NN = (((1,), (0,)), ((), ()))


def mm(a, b, dims):
    return lax.dot_general(a, b, dims, preferred_element_type=jnp.float32)


def rows_of(i, n):
    return pl.ds(pl.multiple_of(i * n, n), n)


def in_order(core, mine, other, dst):
    half = dst.shape[0] // 2
    dst[rows_of(core, half), :] = mine
    dst[rows_of(1 - core, half), :] = other


def terms(kb, vb, qb, dob, rows, starts, c1, k_pos, q_pos):
    shape = (kb.shape[0], qb.shape[0])
    s = mm(kb, qb, NT)
    dp = mm(vb, dob, NT)
    kp = k_pos + lax.broadcasted_iota(jnp.int32, shape, 0)
    vis = kp >= starts
    if q_pos is not None:
        vis = vis & (kp <= q_pos + lax.broadcasted_iota(jnp.int32, shape, 1))
    p = jnp.where(vis, jnp.exp2(s * c1 - rows[0:1, :]), 0.0)
    ds = (p * (dp - rows[1:2, :])).astype(jnp.bfloat16)
    return p.astype(jnp.bfloat16), ds


def sweep(tab, item, count, off, unroll):
    def several(t, n):
        todo = []
        for u in range(n):
            code = tab[off + t + u]
            todo += item(code // 256, lax.rem(code, 256))
        for acc, sl, val in todo:
            acc[sl] += val

    full = count // unroll

    def step(t, _):
        several(t * unroll, unroll)
        return 0

    def single(t, _):
        several(t, 1)
        return 0

    lax.fori_loop(0, full, step, 0)
    if unroll > 1:
        lax.fori_loop(full * unroll, count, single, 0)


def local_kernel(scale, n_list, tab, q_m, k_m, v_m, do_m, oth, st, qs, dq_o, dk_o, dv_o, q, k, v, do, k_t):
    tok = q.shape[0]
    base, core = tab[0], tab[1]
    for n, (mine, dst) in enumerate(((k_m, k), (v_m, v), (q_m, q), (do_m, do))):
        in_order(core, mine[0], oth[n, 0], dst)
    dq_o[...] = jnp.zeros_like(dq_o)
    dk_o[...] = jnp.zeros_like(dk_o)
    dv_o[...] = jnp.zeros_like(dv_o)
    for j in range(tok // KB):
        k_t[j] = jnp.transpose(k[j * KB : (j + 1) * KB, :])

    def item(i, j):
        ks, sl = rows_of(j, KB), rows_of(i, QB)
        qb, dob = q[sl, :], do[sl, :]
        p, ds = terms(k[ks, :], v[ks, :], qb, dob, st[0, i], qs[i], scale * LOG2E, base + j * KB, base + i * QB)
        return [(dv_o.at[0], ks, mm(p, dob, NN)), (dk_o.at[0], ks, mm(ds, qb, NN)), (dq_o.at[0], i, mm(k_t[j], ds, NN))]

    sweep(tab, item, tab[2], 5, UNROLL[0])


def cross_kernel(scale, n_loc, kbu, tab, q_m, k_m, v_m, do_m, oth, st, qs, dq_i, dk_i, dv_i, kvu, qdd, std, qsd, *rest):
    dq, dk, dv, send, q, k, v, do, dq_a, dk_a, dv_a, ku_t = rest[-12:]
    tok, reach = q.shape[0], kvu.shape[2]
    half = tok // 2
    base, core = tab[0], tab[1]
    nu, nq = reach // kbu, tok // QB
    for n, (mine, dst) in enumerate(((k_m, k), (v_m, v), (q_m, q), (do_m, do))):
        in_order(core, mine[0], oth[n, 0], dst)
    dq_a[...] = dq_i[0]
    dk_a[...] = dk_i[0]
    dv_a[...] = dv_i[0]
    off_up, off_dn = 5 + n_loc, 5 + n_loc + nq * nu

    def turn(j, _):
        ku_t[j] = jnp.transpose(kvu[0, 0, rows_of(j, kbu), :])
        return 0

    def up_item(i, j):
        sl, ks = rows_of(i, QB), rows_of(j, kbu)
        _, ds = terms(kvu[0, 0, ks, :], kvu[1, 0, ks, :], q[sl, :], do[sl, :], st[0, i], qs[i], scale * LOG2E, base - reach + j * kbu, None)
        return [(dq_a, i, mm(ku_t[j], ds, NN))]

    def dn_item(i, j):
        sl, ks = rows_of(i, QBD), rows_of(j, KB)
        qb, dob = qdd[0, 0, sl, :], qdd[1, 0, sl, :]
        p, ds = terms(k[ks, :], v[ks, :], qb, dob, std[0, i], qsd[i], scale * LOG2E, base + j * KB, None)
        return [(dv_a, ks, mm(p, dob, NN)), (dk_a, ks, mm(ds, qb, NN))]

    lax.fori_loop(jnp.where(tab[3] > 0, lax.rem(tab[off_up], 256), nu), nu, turn, 0)
    sweep(tab, up_item, tab[3], off_up, UNROLL[1])
    sweep(tab, dn_item, tab[4], off_dn, UNROLL[2])
    for i in range(nq):
        sl = slice(i * QB, (i + 1) * QB)
        q[sl, :] = jnp.transpose(dq_a[i] * scale).astype(jnp.bfloat16)
    mine, gone = rows_of(core, half), rows_of(1 - core, half)
    dq[0], send[0, 0] = q[mine, :], q[gone, :]
    for n, (acc, mul, out) in enumerate(((dk_a, scale, dk), (dv_a, None, dv))):
        for rows, dst in ((mine, out.at[0]), (gone, send.at[n + 1, 0])):
            val = acc[rows, :]
            dst[...] = (val if mul is None else val * mul).astype(jnp.bfloat16)


def up_rows(reach):
    return reach // max(1, round(reach / KB))


def pack(seen):
    rows, cols = seen.shape
    code = (jnp.arange(rows)[:, None] * 256 + jnp.arange(cols)[None, :]).reshape(-1)
    flat = seen.reshape(-1)
    rank = jnp.sum(jnp.tril(jnp.broadcast_to(flat[None, :], (flat.size, flat.size)), -1), axis=1)
    slot = jnp.arange(flat.size)[:, None] == rank[None, :]
    return jnp.sum(flat), jnp.sum(jnp.where(slot & flat[None, :], code[None, :], 0), axis=1)


def make_table(start, base, core, tok, reach):
    kbu = up_rows(reach)
    loc = start[:tok].reshape(-1, QB)[:, :1]
    dn = start[tok : tok + reach].reshape(-1, QBD)[:, :1]
    up_end = base - reach + kbu * (jnp.arange(reach // kbu) + 1)
    k_end = base + KB * (jnp.arange(tok // KB) + 1)
    q_end = base + QB * (jnp.arange(tok // QB) + 1)
    causal = (k_end - KB)[None, :] < q_end[:, None]
    lists = [pack((k_end[None, :] > loc) & causal), pack(up_end[None, :] > loc), pack(k_end[None, :] > dn)]
    return jnp.concatenate([jnp.stack([base, core] + [c for c, _ in lists])] + [l for _, l in lists]).astype(jnp.int32)


def send_kernel(tab, q_m, k_m, v_m, do_m, oth, kv, qd):
    half, n = k_m.shape[1], kv.shape[2]
    cut = 2 * half - n
    for core in range(2):
        @pl.when(tab[1] == core)
        def _():
            for a, (k_x, q_x) in enumerate(((k_m, q_m), (v_m, do_m))):
                k_half = (k_x[0], oth[a, 0])[:: 1 - 2 * core]
                q_half = (q_x[0], oth[a + 2, 0])[:: 1 - 2 * core]
                kv[a, 0, : half - cut, :] = k_half[0][cut:]
                kv[a, 0, half - cut :, :] = k_half[1]
                qd[a, 0, :half, :] = q_half[0]
                qd[a, 0, half:, :] = q_half[1][: half - cut]


def solution(mesh):
    cp = mesh.shape["cp"]
    chips = cp // 2
    head_spec = P("cp", "hp", None)
    swap = [(2 * z + c, 2 * z + 1 - c) for z in range(chips) for c in range(2)]
    bf16, f32 = jnp.bfloat16, jnp.float32

    def perm(x, hop):
        return lax.ppermute(x, "cp", [(2 * z + c, 2 * (z + hop) + c) for z in range(chips) if 0 <= z + hop < chips for c in range(2)])

    def device_fn(q_loc, k_loc, v_loc, o_loc, do_loc, lse_loc, cu):
        half, heads, dim = q_loc.shape
        hh, tok, seq = heads // 2, 2 * half, half * cp
        nq, nk = tok // QB, tok // KB
        n_loc = nq * nk
        scale = dim ** -0.5
        me = lax.axis_index("cp")
        core = lax.rem(me, 2)
        base = (me // 2) * tok
        kh, vh, qh, doh, oh = (jnp.transpose(x, (1, 0, 2)) for x in (k_loc, v_loc, q_loc, do_loc, o_loc))

        def part(x, which):
            return lax.dynamic_slice_in_dim(x, which * hh, hh, 0)

        oth = lax.ppermute(jnp.stack([part(x, 1 - core) for x in (kh, vh, qh, doh)]), "cp", swap)
        delta = jnp.sum(doh.astype(f32) * oh.astype(f32), axis=-1)
        st = jnp.stack([jnp.transpose(lse_loc) * LOG2E, delta], axis=1)
        st_m, st_x = part(st, core), lax.ppermute(part(st, 1 - core), "cp", swap)
        st_all = jnp.where(core == 0, jnp.concatenate([st_m, st_x], axis=2), jnp.concatenate([st_x, st_m], axis=2))

        pos = base + jnp.arange(tok + MAX_DOC, dtype=jnp.int32)
        start = jnp.max(jnp.where(cu[None, :] <= pos[:, None], cu[None, :], 0), axis=1)
        start = jnp.where(pos < seq, start, seq).astype(jnp.int32)

        def blocks(x, n):
            return jnp.transpose(x.reshape(hh, 2, -1, n), (0, 2, 1, 3))

        def path(n, far, groups):
            reach = n + far
            kbu, nd = up_rows(reach), reach // QBD
            tab = make_table(start, base, core, tok, reach)
            st_dn = perm(st_all[:, :, :n], -1)
            if far:
                st_dn = jnp.concatenate([st_dn, perm(st_all[:, :, :far], -2)], axis=2)

            def mine_spec(h0):
                return pl.BlockSpec((1, half, dim), lambda h, t: (t[1] * hh + h0 + h, 0, 0))

            def head_spec_of(block, h0):
                zeros = (0,) * (len(block) - 1)
                return pl.BlockSpec(block, lambda h, t: (h0 + h,) + zeros)

            def stack_spec(lead, length, h0):
                return pl.BlockSpec((lead, 1, length, dim), lambda h, t: (0, h0 + h, 0, 0))

            def whole(x):
                return pl.BlockSpec(x.shape, lambda h, t: (0,) * x.ndim)

            def call(kernel, g, ins, outs, scratch, flops, moved, name, alias={}):
                return pl.pallas_call(
                    kernel,
                    grid_spec=pltpu.PrefetchScalarGridSpec(
                        num_scalar_prefetch=1, grid=(g,), in_specs=[s for _, s in ins], out_specs=[s for _, s in outs],
                        scratch_shapes=scratch),
                    out_shape=[s for s, _ in outs],
                    input_output_aliases=alias,
                    compiler_params=pltpu.CompilerParams(dimension_semantics=("arbitrary",), vmem_limit_bytes=44 * 2**20),
                    cost_estimate=pl.CostEstimate(flops=flops, bytes_accessed=moved, transcendentals=0),
                    name=name,
                )(tab, *[x for x, _ in ins])

            def own(h0):
                return [(x, mine_spec(h0)) for x in (qh, kh, vh, doh)] + [(oth, stack_spec(4, half, h0))]

            S = jax.ShapeDtypeStruct
            unit = 2 * tok * tok * dim
            recv, h0 = [], 0
            for g in groups:
                def packed(m):
                    out = (S((2, g, m, dim), bf16), stack_spec(2, m, 0))
                    return call(send_kernel, g, own(h0), [out, out], [], 1000, g * 12 * tok * dim, "pack")
                kv, qd = packed(n)
                kvu, qdd = perm(kv, 1), perm(qd, -1)
                if far:
                    kvf, qdf = kv[:, :, n - far :], qd[:, :, :far]
                    kvu = jnp.concatenate([perm(kvf, 2), kvu], axis=2)
                    qdd = jnp.concatenate([qdd, perm(qdf, -2)], axis=2)
                recv.append((kvu, qdd))
                h0 += g

            stats, starts = blocks(st_all, QB), start[:tok].reshape(-1, 1, QB)
            stats_d, starts_d = blocks(st_dn, QBD), start[tok : tok + reach].reshape(-1, 1, QBD)
            row_in = lambda h0: [(stats, head_spec_of((1, nq, 2, QB), h0)), (starts, whole(starts))]
            sums = [((nq, dim, QB), f32), ((tok, dim), f32), ((tok, dim), f32)]
            in_tok = [pltpu.VMEM((tok, dim), bf16)] * 4
            acc = call(
                functools.partial(local_kernel, scale, n_loc), hh, own(0) + row_in(0),
                [(S((hh,) + s, d), head_spec_of((1,) + s, 0)) for s, d in sums],
                in_tok + [pltpu.VMEM((nk, dim, KB), bf16)], hh * unit * 2, hh * 28 * tok * dim, "local")

            grads, back, h0 = [], [], 0

            def place(grads, h0, got):
                at = (1 - core) * hh + h0
                return [lax.dynamic_update_slice_in_dim(x, got[n], at, 0) for n, x in enumerate(grads)]

            for g, (kvu, qdd) in zip(groups, recv):
                if len(back) > 1:
                    grads = place(grads, *back.pop(0))
                ins = own(h0) + row_in(h0)
                ins += [(a, head_spec_of((1,) + s, h0)) for a, (s, _) in zip(acc, sums)]
                ins += [(kvu, stack_spec(2, reach, 0)), (qdd, stack_spec(2, reach, 0))]
                ins += [(stats_d, head_spec_of((1, nd, 2, QBD), h0)), (starts_d, whole(starts_d))]
                alias = {1 + len(ins) + n: n for n in range(len(grads))}
                ins += [(x, pl.BlockSpec(memory_space=pl.ANY)) for x in grads]
                outs = [(S((heads, half, dim), bf16), mine_spec(h0))] * 3 + [(S((3, g, half, dim), bf16), stack_spec(3, half, 0))]
                *grads, send = call(
                    functools.partial(cross_kernel, scale, n_loc, kbu), g, ins, outs,
                    in_tok + [pltpu.VMEM(s, d) for s, d in sums] + [pltpu.VMEM((reach // kbu, dim, kbu), bf16)],
                    g * unit * 2, g * 28 * tok * dim, "cross", alias)
                back.append((h0, lax.ppermute(send, "cp", swap)))
                h0 += g
            for item in back:
                grads = place(grads, *item)
            return tuple(grads)

        edge = tok * jnp.arange(1, chips, dtype=jnp.int32)
        e_start = jnp.max(jnp.where(cu[None, :] < edge[:, None], cu[None, :], 0), axis=1)
        e_end = jnp.min(jnp.where(cu[None, :] >= edge[:, None], cu[None, :], seq), axis=1)
        need = jnp.max(jnp.where(e_end > edge, jnp.maximum(edge - e_start, e_end - edge), 0))
        branch = (need > NARROW).astype(jnp.int32) + (need > tok).astype(jnp.int32)
        outs = lax.switch(branch, [lambda: path(NARROW, 0, GROUPS), lambda: path(tok, 0, (3, 3)), lambda: path(tok, MAX_DOC - tok, (hh,))])
        return tuple(jnp.transpose(x, (1, 0, 2)) for x in outs)

    specs = (head_spec,) * 5 + (P("cp", "hp"), P())
    return jax.shard_map(device_fn, mesh=mesh, in_specs=specs, out_specs=(head_spec,) * 3, check_vma=False)
```

```python
import functools
import math

import jax
import jax.numpy as jnp
from jax import lax
from jax.experimental import pallas as pl
from jax.experimental.pallas import tpu as pltpu
from jax.sharding import PartitionSpec as P

LOG2E = math.log2(math.e)
QB = 512
KB = 512
UNROLL = (2, 2, 2)
GROUPS = (3, 3)
NT = (((1,), (1,)), ((), ()))
NN = (((1,), (0,)), ((), ()))


def mm(a, b, dims):
    return lax.dot_general(a, b, dims, preferred_element_type=jnp.float32)


def rows_of(i, n):
    return pl.ds(pl.multiple_of(i * n, n), n)


def in_order(core, mine, other, dst, off=0):
    half = mine.shape[0]
    dst[pl.ds(pl.multiple_of(off + core * half, half), half), :] = mine
    dst[pl.ds(pl.multiple_of(off + (1 - core) * half, half), half), :] = other


def terms(kb, vb, qb, dob, rows, starts, c1, k_pos, q_pos):
    shape = (kb.shape[0], qb.shape[0])
    s = mm(kb, qb, NT)
    dp = mm(vb, dob, NT)
    kp = k_pos + lax.broadcasted_iota(jnp.int32, shape, 0)
    vis = kp >= starts
    if q_pos is not None:
        vis = vis & (kp <= q_pos + lax.broadcasted_iota(jnp.int32, shape, 1))
    p = jnp.where(vis, jnp.exp2(s * c1 - rows[0:1, :]), 0.0)
    ds = (p * (dp - rows[1:2, :])).astype(jnp.bfloat16)
    return p.astype(jnp.bfloat16), ds


def sweep(tab, item, count, off, unroll):
    def several(t, n):
        todo = []
        for u in range(n):
            code = tab[off + t + u]
            todo += item(code // 256, lax.rem(code, 256))
        for acc, sl, val in todo:
            acc[sl] += val

    full = count // unroll

    def step(t, _):
        several(t * unroll, unroll)
        return 0

    def single(t, _):
        several(t, 1)
        return 0

    lax.fori_loop(0, full, step, 0)
    if unroll > 1:
        lax.fori_loop(full * unroll, count, single, 0)


def local_kernel(scale, tab, q_m, k_m, v_m, do_m, kv_x, qd_x, st, qs, *rest):
    dq_o, dk_o, dv_o, q, k, v, do, k_t = rest[-8:]
    tok = q.shape[0]
    base, core = tab[0], tab[1]
    for mine, other, dst in ((k_m, kv_x.at[0], k), (v_m, kv_x.at[1], v), (q_m, qd_x.at[0], q), (do_m, qd_x.at[1], do)):
        in_order(core, mine[0], other[0], dst)
    dq_o[...] = jnp.zeros_like(dq_o)
    dk_o[...] = jnp.zeros_like(dk_o)
    dv_o[...] = jnp.zeros_like(dv_o)
    for j in range(tok // KB):
        k_t[j] = jnp.transpose(k[j * KB : (j + 1) * KB, :])

    def item(i, j):
        ks, sl = rows_of(j, KB), rows_of(i, QB)
        qb, dob = q[sl, :], do[sl, :]
        p, ds = terms(k[ks, :], v[ks, :], qb, dob, st[0, i], qs[i], scale * LOG2E, base + j * KB, base + i * QB)
        return [(dv_o.at[0], ks, mm(p, dob, NN)), (dk_o.at[0], ks, mm(ds, qb, NN)), (dq_o.at[0], i, mm(k_t[j], ds, NN))]

    sweep(tab, item, tab[2], 5, UNROLL[0])


def cross_kernel(scale, n_loc, far, tab, q_m, k_m, v_m, do_m, kv_x, qd_x, st, qs, dq_i, dk_i, dv_i, std, qsd, kv_e, kv_f, qd_e, qd_f, *rest):
    dq, dk, dv, send, q, k, v, do, dq_a, dk_a, dv_a, ku, vu, qd, dod, ku_t = rest[-16:]
    tok, reach = q.shape[0], ku.shape[0]
    half = tok // 2
    base, core = tab[0], tab[1]
    nu, nq = reach // KB, tok // QB
    for mine, other, dst in ((k_m, kv_x.at[0], k), (v_m, kv_x.at[1], v), (q_m, qd_x.at[0], q), (do_m, qd_x.at[1], do)):
        in_order(core, mine[0], other[0], dst)
    for n, (up, dn) in enumerate(((ku, qd), (vu, dod))):
        in_order(core, kv_e[n, 0], kv_f[n, 0], up, far)
        in_order(core, qd_e[n, 0], qd_f[n, 0], dn)
        if far:
            up[:far, :] = rest[0][n, 0]
            dn[tok:, :] = rest[1][n, 0]
    dq_a[...] = dq_i[0]
    dk_a[...] = dk_i[0]
    dv_a[...] = dv_i[0]
    off_up, off_dn = 5 + n_loc, 5 + n_loc + nq * nu

    def turn(j, _):
        ku_t[j] = jnp.transpose(ku[rows_of(j, KB), :])
        return 0

    def up_item(i, j):
        sl, ks = rows_of(i, QB), rows_of(j, KB)
        _, ds = terms(ku[ks, :], vu[ks, :], q[sl, :], do[sl, :], st[0, i], qs[i], scale * LOG2E, base - reach + j * KB, None)
        return [(dq_a, i, mm(ku_t[j], ds, NN))]

    def dn_item(i, j):
        sl, ks = rows_of(i, QB), rows_of(j, KB)
        qb, dob = qd[sl, :], dod[sl, :]
        p, ds = terms(k[ks, :], v[ks, :], qb, dob, std[0, i], qsd[i], scale * LOG2E, base + j * KB, None)
        return [(dv_a, ks, mm(p, dob, NN)), (dk_a, ks, mm(ds, qb, NN))]

    lax.fori_loop(jnp.where(tab[3] > 0, lax.rem(tab[off_up], 256), nu), nu, turn, 0)
    sweep(tab, up_item, tab[3], off_up, UNROLL[1])
    sweep(tab, dn_item, tab[4], off_dn, UNROLL[2])
    for i in range(nq):
        sl = slice(i * QB, (i + 1) * QB)
        q[sl, :] = jnp.transpose(dq_a[i] * scale).astype(jnp.bfloat16)
    mine, gone = rows_of(core, half), rows_of(1 - core, half)
    dq[0], send[0, 0] = q[mine, :], q[gone, :]
    for n, (acc, mul, out) in enumerate(((dk_a, scale, dk), (dv_a, None, dv))):
        for rows, dst in ((mine, out.at[0]), (gone, send.at[n + 1, 0])):
            val = acc[rows, :]
            dst[...] = (val if mul is None else val * mul).astype(jnp.bfloat16)


def pack(seen):
    rows, cols = seen.shape
    code = (jnp.arange(rows)[:, None] * 256 + jnp.arange(cols)[None, :]).reshape(-1)
    flat = seen.reshape(-1)
    rank = jnp.sum(jnp.tril(jnp.broadcast_to(flat[None, :], (flat.size, flat.size)), -1), axis=1)
    slot = jnp.arange(flat.size)[:, None] == rank[None, :]
    return jnp.sum(flat), jnp.sum(jnp.where(slot & flat[None, :], code[None, :], 0), axis=1)


def make_table(start, base, core, tok, reach):
    loc = start[:tok].reshape(-1, QB)[:, :1]
    dn = start[tok : tok + reach].reshape(-1, QB)[:, :1]
    up_end = base - reach + KB * (jnp.arange(reach // KB) + 1)
    k_end = base + KB * (jnp.arange(tok // KB) + 1)
    q_end = base + QB * (jnp.arange(tok // QB) + 1)
    causal = (k_end - KB)[None, :] < q_end[:, None]
    lists = [pack((k_end[None, :] > loc) & causal), pack(up_end[None, :] > loc), pack(k_end[None, :] > dn)]
    return jnp.concatenate([jnp.stack([base, core] + [c for c, _ in lists])] + [l for _, l in lists]).astype(jnp.int32)


def solution(mesh):
    cp = mesh.shape["cp"]
    chips = cp // 2
    head_spec = P("cp", "hp", None)
    bf16, f32 = jnp.bfloat16, jnp.float32

    def perm(x, hop, flip, cores=(0, 1)):
        pairs = [(2 * z + c, 2 * (z + hop) + (c ^ flip)) for z in range(chips) if 0 <= z + hop < chips for c in cores]
        return lax.ppermute(x, "cp", pairs)

    def device_fn(q_loc, k_loc, v_loc, o_loc, do_loc, lse_loc, cu):
        half, heads, dim = q_loc.shape
        hh, tok, seq = heads // 2, 2 * half, half * cp
        nq, nk = tok // QB, tok // KB
        scale = dim ** -0.5
        me = lax.axis_index("cp")
        core = lax.rem(me, 2)
        base = (me // 2) * tok
        kh, vh, qh, doh, oh = (jnp.transpose(x, (1, 0, 2)) for x in (k_loc, v_loc, q_loc, do_loc, o_loc))

        def own_heads(xs, h0, g):
            return jnp.stack([lax.dynamic_slice_in_dim(x, core * hh + h0, g, 0) for x in xs])

        def partner_heads(xs, h0, g):
            return jnp.stack([lax.dynamic_slice_in_dim(x, (1 - core) * hh + h0, g, 0) for x in xs])

        def tokens_in_order(same, other):
            return jnp.where(core == 0, jnp.concatenate([same, other], axis=-1), jnp.concatenate([other, same], axis=-1))

        def path(far, groups):
            reach = tok + far
            n_loc = nq * nk
            delta = jnp.sum(doh.astype(f32) * oh.astype(f32), axis=-1)
            st = jnp.stack([jnp.transpose(lse_loc) * LOG2E, delta], axis=1)
            st_m, st_x = own_heads([st], 0, hh)[0], partner_heads([st], 0, hh)[0]
            st_all = tokens_in_order(st_m, perm(st_x, 0, 1))
            st_dn = tokens_in_order(perm(st_m, -1, 0), perm(st_x, -1, 1))
            if far:
                st_dn = jnp.concatenate([st_dn, jnp.where(core == 0, perm(st_m, -2, 0, (0,)), perm(st_x, -2, 1, (0,)))], axis=-1)

            pos = base + jnp.arange(tok + reach, dtype=jnp.int32)
            start = jnp.max(jnp.where(cu[None, :] <= pos[:, None], cu[None, :], 0), axis=1)
            start = jnp.where(pos < seq, start, seq).astype(jnp.int32)
            tab = make_table(start, base, core, tok, reach)

            recv, sent, h0 = [], [], 0
            kv_in, qd_in = (kh, vh), (qh, doh)
            for n, g in enumerate(groups):
                if n == 1:
                    kv_in, qd_in, st_dn = lax.optimization_barrier((kv_in, qd_in, st_dn))
                kv_m, kv_x, qd_m, qd_x = (f(xs, h0, g) for xs in (kv_in, qd_in) for f in (own_heads, partner_heads))
                got = [perm(kv_x, 0, 1), perm(qd_x, 0, 1)]
                got += [perm(kv_m, 1, 0), perm(kv_x, 1, 1), perm(qd_m, -1, 0), perm(qd_x, -1, 1)]
                if far:
                    got += [jnp.where(core == 1, perm(kv_m, 2, 0, (1,)), perm(kv_x, 2, 1, (1,)))]
                    got += [jnp.where(core == 0, perm(qd_m, -2, 0, (0,)), perm(qd_x, -2, 1, (0,)))]
                recv.append(got)
                sent += [kv_m, qd_m]
                h0 += g

            def mine_spec(h0):
                return pl.BlockSpec((1, half, dim), lambda h, t: (t[1] * hh + h0 + h, 0, 0))

            def row_spec(block, h0):
                zeros = (0,) * (len(block) - 1)
                return pl.BlockSpec((1,) + block, lambda h, t: (h0 + h,) + zeros + (0,))

            def stack_spec(lead):
                return pl.BlockSpec((lead, 1, half, dim), lambda h, t: (0, h, 0, 0))

            def whole(x):
                return pl.BlockSpec(x.shape, lambda h, t: (0,) * x.ndim)

            def call(kernel, g, ins, outs, scratch, name, alias):
                unit = g * tok * dim
                return pl.pallas_call(
                    kernel,
                    grid_spec=pltpu.PrefetchScalarGridSpec(
                        num_scalar_prefetch=1, grid=(g,), in_specs=[s for _, s in ins], out_specs=[s for _, s in outs],
                        scratch_shapes=scratch),
                    out_shape=[s for s, _ in outs],
                    input_output_aliases=alias,
                    compiler_params=pltpu.CompilerParams(dimension_semantics=("arbitrary",), vmem_limit_bytes=48 * 2**20),
                    cost_estimate=pl.CostEstimate(flops=4 * tok * unit, bytes_accessed=28 * unit, transcendentals=0),
                    name=name,
                )(tab, *[x for x, _ in ins])

            S = jax.ShapeDtypeStruct
            anywhere = pl.BlockSpec(memory_space=pl.ANY)

            def blocks(x):
                return jnp.transpose(x.reshape(hh, 2, -1, QB), (0, 2, 1, 3))

            stats, starts = blocks(st_all), start[:tok].reshape(-1, 1, QB)
            stats_d, starts_d = blocks(st_dn), start[tok:].reshape(-1, 1, QB)
            sums = [((nq, dim, QB), f32), ((tok, dim), f32), ((tok, dim), f32)]
            in_tok = [pltpu.VMEM((tok, dim), bf16)] * 4
            in_reach = [pltpu.VMEM((reach, dim), bf16)] * 4

            def common(h0, got):
                ins = [(x, mine_spec(h0)) for x in (qh, kh, vh, doh)] + [(x, stack_spec(2)) for x in got[:2]]
                return ins + [(stats, row_spec((nq, 2, QB), h0)), (starts, whole(starts))]

            parts, h0 = [], 0
            for n, (g, got) in enumerate(zip(groups, recv)):
                ins = common(h0, got) + ([(x, anywhere) for x in sent] if n == 0 else [])
                parts.append(call(
                    functools.partial(local_kernel, scale), g, ins, [(S((g,) + s, d), row_spec(s, 0)) for s, d in sums],
                    in_tok + [pltpu.VMEM((nk, dim, KB), bf16)], "local", {}))
                h0 += g

            grads, back, h0 = [], [], 0

            def place(grads, h0, got):
                at = (1 - core) * hh + h0
                return [lax.dynamic_update_slice_in_dim(x, got[n], at, 0) for n, x in enumerate(grads)]

            for g, got, acc in zip(groups, recv, parts):
                if len(back) > 1:
                    grads = place(grads, *back.pop(0))
                ins = common(h0, got) + [(a, row_spec(s, 0)) for a, (s, _) in zip(acc, sums)]
                ins += [(stats_d, row_spec((reach // QB, 2, QB), h0)), (starts_d, whole(starts_d))]
                ins += [(x, stack_spec(2)) for x in got[2:]]
                alias = {1 + len(ins) + n: n for n in range(len(grads))}
                ins += [(x, anywhere) for x in grads]
                outs = [(S((heads, half, dim), bf16), mine_spec(h0))] * 3 + [(S((3, g, half, dim), bf16), stack_spec(3))]
                *grads, send = call(
                    functools.partial(cross_kernel, scale, n_loc, far), g, ins, outs,
                    in_tok + [pltpu.VMEM(s, d) for s, d in sums] + in_reach + [pltpu.VMEM((reach // KB, dim, KB), bf16)],
                    "cross", alias)
                back.append((h0, perm(send, 0, 1)))
                h0 += g
            for item in back:
                grads = place(grads, *item)
            return tuple(grads)

        edge = tok * jnp.arange(1, chips, dtype=jnp.int32)
        e_start = jnp.max(jnp.where(cu[None, :] < edge[:, None], cu[None, :], 0), axis=1)
        e_end = jnp.min(jnp.where(cu[None, :] >= edge[:, None], cu[None, :], seq), axis=1)
        need = jnp.max(jnp.where(e_end > edge, jnp.maximum(edge - e_start, e_end - edge), 0))
        outs = lax.cond(need > tok, lambda: path(half, (hh,)), lambda: path(0, GROUPS))
        return tuple(jnp.transpose(x, (1, 0, 2)) for x in outs)

    specs = (head_spec,) * 5 + (P("cp", "hp"), P())
    return jax.shard_map(device_fn, mesh=mesh, in_specs=specs, out_specs=(head_spec,) * 3, check_vma=False)
```
